32 devices in a mesh: rep: 2 (over y), gx: 16 (over z, x, core).
Axes of the slice: x: 2, y: 2, z: 4, core: 2. Of those that a mesh axis runs over, the one named last changes fastest.
Arguments:
- positions: float32 [3, 49152], P(None, ('rep', 'gx')), parts along dimension 1, may hold values from 0 to 96
- velocities: float32 [3, 49152], P(None, ('rep', 'gx')), parts along dimension 1, may hold values from -9 to 9
- atom_params: float32 [4, 49152], P(None, ('rep', 'gx')), parts along dimension 1, may hold values from -1 to 2, as said below
- pair_list: int32 [3, 540672], P(None, ('rep', 'gx')), parts along dimension 1, may hold values from 0 to 479, as said below
- pair_count: int32 [32], P(('rep', 'gx')), parts along dimension 0, may hold values from 2112 to 16896, as said below
- exclusion: int32 [4, 540672], P(None, ('rep', 'gx')), parts along dimension 1, may hold values from 0 to 65535, as said below
- halo_far: int32 [3072], P(('rep', 'gx')), parts along dimension 0, may hold values from 0 to 191, as said below
- box_lengths: float32 [6], P('rep'), parts along dimension 0, may hold values from 12 to 96
- extended_variables: float32 [8], P('rep'), parts along dimension 0, may hold values from -0.3 to 0.3
Outputs:
- forces: float32 [3, 49152], P(None, ('rep', 'gx')), parts along dimension 1
- new_velocities: float32 [3, 49152], P(None, ('rep', 'gx')), parts along dimension 1
- new_positions: float32 [3, 49152], P(None, ('rep', 'gx')), parts along dimension 1
- new_coupling: float32 [8], P('rep'), parts along dimension 0
The draws below stay inside these ranges and needn't reach their ends.
There are 2 independent parts, one for each index of `rep`. The reference program is written for one: setup_inputs(seed, part) draws one part's arguments, and reference() takes and returns one part's arrays. A program takes and returns all parts, laid end to end along the dimension named above; each array names one. Nothing has to cross between parts.
Inputs may be any that keep to these rules, and one draw needn't show every extreme that they name: `pair_list`: row 0 is a local cluster 0 to 191, row 1 a slot 0 to 479 of the slot table, row 2 an image code 0 to 8. Over each domain's used columns row 0 never falls (the list is grouped by its first cluster). Unused columns hold valid entries too. `pair_count`: at most 16896; some domain uses all 16896 columns in every draw. `exclusion`: each word holds 16 bits; bit 1 means the atom pair interacts. `halo_far`: 96 distinct local clusters of each domain. `atom_params`: rows 1 to 3 are positive.
All inputs are finite; a program needn't handle non-finite values.
Results may differ from the reference program's by a relative error of at most 0.0003.
Values sent between devices are 32-bit elements; how exact they have to be, the bound alone decides.
A program may use at most 64 MiB of HBM per device.

```python
import math
import jax
import jax.numpy as jnp
import numpy as np
from jax import lax

LX = 2
LY = 12
LZ = 8
CAND = 88
ATOMS_DEV = 1536
PAIRS_DEV = 16896
COPY_PARTICLES = 24576
PAIRS = 270336
N_GX = 16


def candidate_offsets():
    result = [(0, 0, 0)]
    for shift_y in range(-2, 3):
        for shift_z in range(-2, 3):
            if shift_y > 0 or (shift_y == 0 and shift_z > 0):
                result.append((0, shift_y, shift_z))
    for shift_x in range(1, 4):
        for shift_y in range(-2, 3):
            for shift_z in range(-2, 3):
                result.append((shift_x, shift_y, shift_z))
    return np.array(result, np.int32)


def upper_words():
    result = []
    for word_place in range(4):
        packed_bits = 0
        for bit_place in range(16):
            number = word_place * 16 + bit_place
            if number % 8 > number // 8:
                packed_bits += 1 << bit_place
        result.append(packed_bits)
    return np.array(result, np.int32)


def cluster_sites(key):
    subkeys = jax.random.split(jax.random.fold_in(key, 101), N_GX)
    return jax.vmap(lambda single: jax.random.permutation(single, LX * LY * LZ))(subkeys).astype(jnp.int32)


def box_stretch(key):
    return jax.random.uniform(jax.random.fold_in(key, 202), (3,), jnp.float32, -0.02, 0.02)


def pair_counts(key):
    base_counts = jax.random.randint(jax.random.fold_in(key, 303), (N_GX,), PAIRS_DEV // 8, PAIRS_DEV // 2 + 1)
    dense_counts = jax.random.randint(jax.random.fold_in(key, 304), (N_GX,), 3 * PAIRS_DEV // 4, PAIRS_DEV + 1)
    dense_start = jax.random.randint(jax.random.fold_in(key, 305), (), 0, N_GX)
    distance = (jnp.arange(N_GX, dtype=jnp.int32) - dense_start) % N_GX
    counts = jnp.where(distance < max(N_GX // 8, 1), dense_counts, base_counts)
    return jnp.where(distance == 0, PAIRS_DEV, counts).astype(jnp.int32)


def pair_order(key):
    counts = pair_counts(key)
    subkeys = jax.random.split(jax.random.fold_in(key, 306), N_GX)
    ranks = jax.vmap(lambda single: jax.random.permutation(single, PAIRS_DEV))(subkeys)
    candidate = jnp.arange(PAIRS_DEV, dtype=jnp.int32)[None, :]
    sort_key = jnp.where(ranks < counts[:, None], candidate, candidate + PAIRS_DEV)
    return jnp.argsort(sort_key, axis=1).astype(jnp.int32)


def pair_tables(key):
    site_of = cluster_sites(key)
    cluster_at = jnp.argsort(site_of, axis=1).astype(jnp.int32)
    plane_size = LY * LZ
    clusters = LX * plane_size
    offsets = jnp.asarray(candidate_offsets())
    layer_x = (site_of // plane_size)[:, :, None]
    layer_y = (site_of // LZ % LY)[:, :, None]
    layer_z = (site_of % LZ)[:, :, None]
    target_x = layer_x + offsets[:, 0]
    raw_y = layer_y + offsets[:, 1]
    raw_z = layer_z + offsets[:, 2]
    wrap_y = (raw_y >= LY).astype(jnp.int32) - (raw_y < 0).astype(jnp.int32)
    wrap_z = (raw_z >= LZ).astype(jnp.int32) - (raw_z < 0).astype(jnp.int32)
    target_y = raw_y - wrap_y * LY
    target_z = raw_z - wrap_z * LZ
    image_code = (wrap_y + 1) * 3 + wrap_z + 1
    in_plane = target_y * LZ + target_z
    own_site = jnp.clip(target_x, 0, LX - 1) * plane_size + in_plane
    near_site = jnp.clip(target_x - LX, 0, LX - 1) * plane_size + in_plane
    next_at = jnp.roll(cluster_at, -1, axis=0)
    own_slot = jnp.take_along_axis(cluster_at, own_site.reshape(N_GX, -1), axis=1).reshape(own_site.shape)
    near_slot = clusters + jnp.take_along_axis(next_at, near_site.reshape(N_GX, -1), axis=1).reshape(near_site.shape)
    far_slot = 2 * clusters + in_plane
    second = jnp.where(target_x < LX, own_slot, jnp.where(target_x < 2 * LX, near_slot, far_slot))
    first = jnp.broadcast_to(jnp.arange(clusters, dtype=jnp.int32)[None, :, None], second.shape)
    is_self = jnp.broadcast_to((jnp.arange(CAND) == 0)[None, None, :], second.shape)
    tables = jnp.stack([first, second, image_code]).reshape(3, N_GX, clusters * CAND).astype(jnp.int32)
    return (tables, is_self.reshape(N_GX, clusters * CAND))


def draw_positions(key, part):
    site_of = cluster_sites(key)
    stretch = box_stretch(key)
    plane_size = LY * LZ
    layer_x = (site_of // plane_size)[:, :, None]
    layer_y = (site_of // LZ % LY)[:, :, None]
    layer_z = (site_of % LZ)[:, :, None]
    atom_slot = jnp.arange(8, dtype=jnp.int32)
    domain = jnp.arange(N_GX, dtype=jnp.int32)[:, None, None]
    coord_x = (domain * LX + layer_x) * 2 + atom_slot // 4
    coord_y = layer_y * 2 + atom_slot // 2 % 2
    coord_z = layer_z * 2 + atom_slot % 2
    lattice = jnp.stack([coord_x, coord_y, coord_z]).astype(jnp.float32).reshape(3, COPY_PARTICLES) + 0.5
    jitter = jax.random.uniform(jax.random.fold_in(key, 203), (3, COPY_PARTICLES), jnp.float32, -0.05, 0.05)
    return lattice * (1.0 + stretch[:, None]) + jitter


def draw_box_lengths(key, part):
    nominal = jnp.array([2.0 * LX * N_GX, 2.0 * LY, 2.0 * LZ], jnp.float32)
    return nominal * (1.0 + box_stretch(key))


def draw_velocities(key, part):
    domain = (jnp.arange(COPY_PARTICLES, dtype=jnp.int32) // ATOMS_DEV).astype(jnp.float32)
    spread = jnp.sqrt(1.0 + 2.0 * domain / (N_GX - 1))
    base = jnp.clip(jax.random.normal(jax.random.fold_in(key, 501), (3, COPY_PARTICLES), jnp.float32), -5.0, 5.0)
    return base * spread[None, :]


def draw_atom_params(key, part):
    charge = jax.random.uniform(jax.random.fold_in(key, 601), (COPY_PARTICLES,), jnp.float32, -1.0, 1.0)
    dispersion = jnp.exp(jax.random.uniform(jax.random.fold_in(key, 602), (COPY_PARTICLES,), jnp.float32, math.log(0.3), 0.0))
    repulsion = jnp.exp(jax.random.uniform(jax.random.fold_in(key, 603), (COPY_PARTICLES,), jnp.float32, math.log(0.1), math.log(0.3)))
    inverse_mass = jnp.exp(jax.random.uniform(jax.random.fold_in(key, 604), (COPY_PARTICLES,), jnp.float32, math.log(0.5), math.log(2.0)))
    return jnp.stack([charge, dispersion, repulsion, inverse_mass])


def draw_pair_list(key, part):
    tables, is_self = pair_tables(key)
    order = pair_order(key)
    return jnp.take_along_axis(tables, order[None, :, :], axis=2).reshape(3, PAIRS)


def draw_pair_count(key, part):
    return pair_counts(key)


def draw_exclusion(key, part):
    tables, is_self = pair_tables(key)
    order = pair_order(key)
    first_words = jax.random.randint(jax.random.fold_in(key, 401), (4, N_GX, PAIRS_DEV), 0, 65536)
    second_words = jax.random.randint(jax.random.fold_in(key, 402), (4, N_GX, PAIRS_DEV), 0, 65536)
    words = first_words | second_words
    upper = jnp.asarray(upper_words())[:, None, None]
    words = jnp.where(is_self[None, :, :], words & upper, words)
    return jnp.take_along_axis(words, order[None, :, :], axis=2).reshape(4, PAIRS).astype(jnp.int32)


def draw_halo_far(key, part):
    site_of = cluster_sites(key)
    cluster_at = jnp.argsort(site_of, axis=1).astype(jnp.int32)
    return cluster_at[:, :LY * LZ].reshape(N_GX * LY * LZ)


def setup_inputs(seed: int = 0, part: int = 0) -> dict:
    seeds = jax.random.split(jax.random.key(seed), 10)
    part_keys = jax.random.split(jax.random.fold_in(seeds[9], part), 10)
    return {
        "positions": draw_positions(jax.random.fold_in(jax.random.fold_in(seeds[9], part), 71), part),
        "velocities": draw_velocities(jax.random.fold_in(jax.random.fold_in(seeds[9], part), 71), part),
        "atom_params": draw_atom_params(jax.random.fold_in(jax.random.fold_in(seeds[9], part), 71), part),
        "pair_list": draw_pair_list(jax.random.fold_in(jax.random.fold_in(seeds[9], part), 71), part),
        "pair_count": draw_pair_count(jax.random.fold_in(jax.random.fold_in(seeds[9], part), 71), part),
        "exclusion": draw_exclusion(jax.random.fold_in(jax.random.fold_in(seeds[9], part), 71), part),
        "halo_far": draw_halo_far(jax.random.fold_in(jax.random.fold_in(seeds[9], part), 71), part),
        "box_lengths": draw_box_lengths(jax.random.fold_in(jax.random.fold_in(seeds[9], part), 71), part),
        "extended_variables": jnp.clip(jax.random.uniform(part_keys[8], (4,), jnp.float32, -0.3, 0.3), -0.3, 0.3),
    }


time_step = 0.25
reaction_term = 1.0 / 1331.0
thermal_scale_unit = 2.0
reservoir_inertia_mass = 4.0
barostat_gain = 0.1
pressure_target = 1.0

def pair_tiles(slot_table, pair_rows, word_rows, usable, box_lengths):
    tile_width = pair_rows.shape[1]
    first_rows = jnp.take(slot_table, pair_rows[0], axis=0).T.reshape(6, 8, tile_width)
    second_rows = jnp.take(slot_table, pair_rows[1], axis=0).T.reshape(6, 8, tile_width)
    image_y = (pair_rows[2] // 3 - 1).astype(jnp.float32) * box_lengths[1]
    image_z = (pair_rows[2] % 3 - 1).astype(jnp.float32) * box_lengths[2]
    delta_x = second_rows[0][None, :, :] - first_rows[0][:, None, :]
    delta_y = second_rows[1][None, :, :] - first_rows[1][:, None, :] + image_y
    delta_z = second_rows[2][None, :, :] - first_rows[2][:, None, :] + image_z
    shifts = (jnp.arange(64, dtype=jnp.int32) % 16)[:, None]
    mask_bits = jnp.right_shift(jnp.repeat(word_rows, 16, axis=0), shifts) & 1
    interact = (mask_bits.reshape(8, 8, tile_width) == 1) & usable[None, None, :]
    radius_sq = delta_x * delta_x + delta_y * delta_y + delta_z * delta_z
    radius_sq = jnp.where(interact, radius_sq, 1.0)
    inverse = lax.rsqrt(radius_sq)
    inverse_sq = inverse * inverse
    inverse_six = inverse_sq * inverse_sq * inverse_sq
    charge_pair = first_rows[3][:, None, :] * second_rows[3][None, :, :]
    dispersion = first_rows[4][:, None, :] * second_rows[4][None, :, :]
    repulsion = first_rows[5][:, None, :] * second_rows[5][None, :, :]
    scalar = charge_pair * (inverse * inverse_sq - reaction_term) + (12.0 * repulsion * inverse_six - 6.0 * dispersion) * inverse_six * inverse_sq
    scalar = jnp.where(interact, scalar, 0.0)
    components = (delta_x, delta_y, delta_z)
    onto_second = jnp.stack([lax.optimization_barrier(jnp.sum(scalar * component, axis=0)) for component in components])
    onto_first = -jnp.stack([lax.optimization_barrier(jnp.sum(scalar * component, axis=1)) for component in components])
    virial = -0.5 * jnp.stack([jnp.sum(scalar * component * component) for component in components])
    tile_terms = jnp.concatenate([onto_first.reshape(24, tile_width), onto_second.reshape(24, tile_width)], axis=1).T
    owners = jnp.concatenate([pair_rows[0], pair_rows[1]])
    return (tile_terms, owners, virial)

def device_forces(slot_table, pair_rows, word_rows, pair_total, box_lengths):
    slots = slot_table.shape[0]
    block_rows = PAIRS_DEV // LY
    starts = jnp.arange(LY, dtype=jnp.int32) * block_rows

    def one_block(running, first_row):
        accumulated, virial = running
        pair_block = lax.dynamic_slice_in_dim(pair_rows, first_row, block_rows, 1)
        word_block = lax.dynamic_slice_in_dim(word_rows, first_row, block_rows, 1)
        usable = first_row + jnp.arange(block_rows, dtype=jnp.int32) < pair_total
        tile_terms, owners, partial_value = pair_tiles(slot_table, pair_block, word_block, usable, box_lengths)
        accumulated = accumulated + jax.ops.segment_sum(tile_terms, owners, num_segments=slots)
        return ((accumulated, virial + partial_value), None)
    start_state = (jnp.zeros((slots, 24), jnp.float32), jnp.zeros((3,), jnp.float32))
    result, unused = lax.scan(one_block, start_state, starts)
    return result

def reference(positions, velocities, atom_params, pair_list, pair_count, exclusion, halo_far, box_lengths, extended_variables):
    clusters = LX * LY * LZ
    far_clusters = LY * LZ
    slots = 2 * clusters + far_clusters
    packed = jnp.concatenate([positions, atom_params[:3]], axis=0)
    packed = packed.reshape(6, N_GX, clusters, 8).transpose(1, 0, 2, 3)
    far_lists = halo_far.reshape(N_GX, far_clusters)
    far_rows = jax.vmap(lambda block_data, chosen: block_data[:, chosen, :])(packed, far_lists)
    domain = jnp.arange(N_GX, dtype=jnp.int32)
    near_rows = jnp.roll(packed, -1, axis=0)
    far_in = jnp.roll(far_rows, -2, axis=0)
    near_lift = jnp.where(domain == N_GX - 1, box_lengths[0], 0.0)
    far_lift = jnp.where(domain >= N_GX - 2, box_lengths[0], 0.0)
    near_rows = near_rows.at[:, 0].add(near_lift[:, None, None])
    far_in = far_in.at[:, 0].add(far_lift[:, None, None])
    tables = jnp.concatenate([packed, near_rows, far_in], axis=2)
    tables = tables.transpose(0, 2, 1, 3).reshape(N_GX, slots, 48)
    pair_blocks = pair_list.reshape(3, N_GX, PAIRS_DEV).transpose(1, 0, 2)
    word_blocks = exclusion.reshape(4, N_GX, PAIRS_DEV).transpose(1, 0, 2)

    def per_domain(item):
        return device_forces(item[0], item[1], item[2], item[3], box_lengths)
    accumulated, virials = lax.map(per_domain, (tables, pair_blocks, word_blocks, pair_count))
    own_part = accumulated[:, :clusters]
    near_back = jnp.roll(accumulated[:, clusters:2 * clusters], 1, axis=0)
    far_back = jnp.roll(accumulated[:, 2 * clusters:], 2, axis=0)
    summed = own_part + near_back
    summed = jax.vmap(lambda block_data, chosen, extra: block_data.at[chosen].add(extra))(summed, far_lists, far_back)
    forces = summed.reshape(N_GX, clusters, 3, 8).transpose(2, 0, 1, 3).reshape(3, COPY_PARTICLES)
    inverse_mass = atom_params[3]
    kinetic = 0.5 * lax.optimization_barrier(jnp.sum(velocities * velocities / inverse_mass[None, :], axis=1))
    virial = lax.optimization_barrier(jnp.sum(virials, axis=0))
    overall_motion_work = jnp.sum(kinetic)
    volume = box_lengths[0] * box_lengths[1] * box_lengths[2]
    thermal_ratio_value = 2.0 * overall_motion_work / (3.0 * COPY_PARTICLES * thermal_scale_unit)
    reservoir_damping = extended_variables[0] + reservoir_inertia_mass * (thermal_ratio_value - 1.0)
    box_rates = extended_variables[1:] + barostat_gain * (kinetic - virial - pressure_target * volume / 2.0) / (overall_motion_work / 3.0)
    new_velocities = velocities + time_step * (forces * inverse_mass[None, :] - (reservoir_damping + box_rates[:, None]) * velocities)
    new_positions = positions * (1.0 + time_step * box_rates[:, None]) + time_step * new_velocities
    new_coupling = jnp.concatenate([reservoir_damping[None], box_rates])
    return (forces, new_velocities, new_positions, new_coupling)
```

```python
import functools

import jax
import jax.numpy as jnp
from jax import lax
from jax.experimental import pallas as pl
from jax.experimental.pallas import tpu as pltpu
from jax.sharding import PartitionSpec as P

time_step = 0.25
reaction_term = 1.0 / 1331.0
thermal_scale_unit = 2.0
reservoir_inertia_mass = 4.0
barostat_gain = 0.1
pressure_target = 1.0

LANES = 128


def passed_along(value, axis, steps):
    count = lax.axis_size(axis)
    pairs = [(source, (source + steps) % count) for source in range(count)]
    return lax.ppermute(value, axis, pairs)


def round_up(value, unit):
    return (value + unit - 1) // unit * unit


def split_three(value):
    high = value.astype(jnp.bfloat16).astype(jnp.float32)
    rest = value - high
    middle = rest.astype(jnp.bfloat16).astype(jnp.float32)
    return jnp.concatenate([high, middle, rest - middle], axis=0).astype(jnp.bfloat16)


def one_hot_rows(index_row, rows, ramp):
    pieces = []
    for base in range(0, rows, 256):
        height = min(256, rows - base)
        moved = (index_row - base).astype(jnp.float32)
        moved = jnp.broadcast_to(moved, (16, LANES)).astype(jnp.bfloat16)
        for first in range(0, height, 16):
            hit = moved == ramp[first : first + 16]
            pieces.append(jnp.where(hit, jnp.bfloat16(1), jnp.bfloat16(0)))
    return jnp.concatenate(pieces, axis=0)


def gathered(table_ref, index_row, tiles):
    index = jnp.broadcast_to(index_row, (8, LANES))
    within = index & (LANES - 1)
    block = index // LANES
    result = []
    for component in range(6):
        value = None
        for tile in range(tiles):
            source = table_ref[component * 8 : component * 8 + 8, tile * LANES : (tile + 1) * LANES]
            picked = jnp.take_along_axis(source, within, axis=1, mode="promise_in_bounds")
            value = picked if value is None else jnp.where(block == tile, picked, value)
        result.append(value)
    return result


def pair_kernel(
    count_ref, box_ref, table_ref, pair_ref, word_ref, own_ref, other_ref, virial_ref,
    first_terms, second_terms, *, clusters, slots, block
):
    sublane = lax.broadcasted_iota(jnp.int32, (8, LANES), 0)
    lane = lax.broadcasted_iota(jnp.int32, (8, LANES), 1)
    ramp = lax.broadcasted_iota(jnp.int32, (256, LANES), 0).astype(jnp.float32).astype(jnp.bfloat16)
    count = count_ref[0]
    box_y = box_ref[1]
    box_z = box_ref[2]
    first_tiles = -(-clusters // LANES)
    second_tiles = -(-slots // LANES)
    own_ref[...] = jnp.zeros_like(own_ref)
    other_ref[...] = jnp.zeros_like(other_ref)
    virial_ref[...] = jnp.zeros_like(virial_ref)

    def one_block(number, carry):
        start = pl.multiple_of(number * block, LANES)
        first_hot = []
        second_hot = []
        virial = [virial_ref[c * 8 : c * 8 + 8, :] for c in range(3)]
        for part in range(block // LANES):
            at = pl.multiple_of(start + part * LANES, LANES)
            here = pl.ds(at, LANES)
            first_row = pair_ref[0:1, here]
            second_row = pair_ref[1:2, here]
            image = jnp.broadcast_to(pair_ref[2:3, here], (8, LANES))
            first = gathered(table_ref, first_row, first_tiles)
            second = gathered(table_ref, second_row, second_tiles)
            step_y = jnp.where(image >= 6, 1.0, jnp.where(image >= 3, 0.0, -1.0))
            step_z = image.astype(jnp.float32) - 3.0 * step_y - 4.0
            shift = (None, step_y * box_y, step_z * box_z)
            for c in range(3):
                origin = jnp.broadcast_to(first[c][0:1], (8, LANES))
                second[c] = second[c] - origin
                if shift[c] is not None:
                    second[c] = second[c] + shift[c]
                first[c] = first[c] - origin
            words = [jnp.broadcast_to(word_ref[w : w + 1, here], (8, LANES)) for w in range(4)]
            low = jnp.where(sublane < 2, words[0], words[1])
            high = jnp.where(sublane < 6, words[2], words[3])
            bits = jnp.where(sublane < 4, low, high) >> (8 * (sublane & 1))
            bits = jnp.where(at + lane < count, bits, 0)
            charge, dispersion, repulsion = first[3], 6.0 * first[4], 12.0 * first[5]
            moving = list(second)
            onto_first = [None] * 3
            onto_second = [None] * 3
            for turn in range(7, -1, -1):
                moving = [pltpu.roll(m, 1, 0) for m in moving] if turn else second
                delta = [moving[c] - first[c] for c in range(3)]
                radius_sq = delta[0] * delta[0] + delta[1] * delta[1] + delta[2] * delta[2]
                inverse = lax.rsqrt(radius_sq)
                inverse_sq = inverse * inverse
                cube = inverse * inverse_sq
                six = cube * cube
                scalar = charge * moving[3] * (cube - reaction_term) + (
                    repulsion * moving[5] * six - dispersion * moving[4]
                ) * (six * inverse_sq)
                wanted = (bits & (1 << ((sublane + turn) & 7))) != 0
                scalar = jnp.where(wanted, scalar, 0.0)
                for c in range(3):
                    force = scalar * delta[c]
                    if onto_first[c] is None:
                        onto_first[c] = -force
                        onto_second[c] = force
                    else:
                        onto_first[c] = onto_first[c] - force
                        onto_second[c] = pltpu.roll(onto_second[c], 1, 0) + force
            for c in range(3):
                virial[c] = virial[c] + (onto_second[c] * second[c] + onto_first[c] * first[c])
            lanes = slice(part * LANES, (part + 1) * LANES)
            first_terms[:, lanes] = split_three(jnp.concatenate(onto_first, axis=0))
            second_terms[:, lanes] = split_three(jnp.concatenate(onto_second, axis=0))
            first_hot.append(one_hot_rows(first_row, clusters, ramp))
            second_hot.append(one_hot_rows(second_row, slots, ramp))
        for c in range(3):
            virial_ref[c * 8 : c * 8 + 8, :] = virial[c]
        contract = (((1,), (1,)), ((), ()))
        own_ref[...] += lax.dot_general(
            jnp.concatenate(first_hot, axis=1), first_terms[...], contract,
            preferred_element_type=jnp.float32,
        )
        other_ref[...] += lax.dot_general(
            jnp.concatenate(second_hot, axis=1), second_terms[...], contract,
            preferred_element_type=jnp.float32,
        )
        return carry

    lax.fori_loop(0, (count + block - 1) // block, one_block, 0)


def pair_forces(pair_count, box_lengths, table, pair_list, exclusion, clusters, slots):
    pairs = pair_list.shape[1]
    block = next(b for b in (512, 384, 256, 128) if pairs % b == 0)
    vmem = pl.BlockSpec(memory_space=pltpu.VMEM)
    smem = pl.BlockSpec(memory_space=pltpu.SMEM)
    return pl.pallas_call(
        functools.partial(pair_kernel, clusters=clusters, slots=slots, block=block),
        out_shape=(
            jax.ShapeDtypeStruct((clusters, 72), jnp.float32),
            jax.ShapeDtypeStruct((slots, 72), jnp.float32),
            jax.ShapeDtypeStruct((24, LANES), jnp.float32),
        ),
        in_specs=[smem, smem, vmem, vmem, vmem],
        out_specs=(vmem, vmem, vmem),
        scratch_shapes=[
            pltpu.VMEM((72, block), jnp.bfloat16),
            pltpu.VMEM((72, block), jnp.bfloat16),
        ],
    )(pair_count, box_lengths, table, pair_list, exclusion)


def on_device(
    positions,
    velocities,
    atom_params,
    pair_list,
    pair_count,
    exclusion,
    halo_far,
    box_lengths,
    extended_variables,
):
    atoms_here = positions.shape[1]
    clusters = atoms_here // 8
    far_clusters = halo_far.shape[0]
    slots = 2 * clusters + far_clusters
    domain_index = lax.axis_index("gx")
    axis_count = lax.axis_size("gx")
    inverse_mass = atom_params[3]
    kinetic = 0.5 * jnp.sum(velocities * velocities / inverse_mass[None, :], axis=1)
    packed = jnp.concatenate([positions, atom_params[:3]], axis=0)
    packed = packed.reshape(6, clusters, 8).transpose(0, 2, 1).reshape(48, clusters)
    far_rows = packed[:, halo_far]
    near_rows = passed_along(packed, "gx", -1)
    far_in = passed_along(far_rows, "gx", -2)
    near_rows = near_rows.at[:8].add(jnp.where(domain_index == axis_count - 1, box_lengths[0], 0.0))
    far_in = far_in.at[:8].add(jnp.where(domain_index >= axis_count - 2, box_lengths[0], 0.0))
    padding = jnp.zeros((48, round_up(slots, LANES) - slots), jnp.float32)
    table = jnp.concatenate([packed, near_rows, far_in, padding], axis=1)
    own, other, virial = pair_forces(
        pair_count, box_lengths, table, pair_list, exclusion, clusters, slots
    )
    other = other[:, :24] + other[:, 24:48] + other[:, 48:]
    near_back = passed_along(other[clusters : 2 * clusters], "gx", 1)
    far_back = passed_along(other[2 * clusters :], "gx", 2)
    own = own[:, :24] + own[:, 24:48] + own[:, 48:] + other[:clusters]
    virial = -0.5 * jnp.sum(virial.reshape(3, 8 * LANES), axis=1)
    kinetic, virial_total = lax.psum((kinetic, virial), "gx")
    summed = (own + near_back).at[halo_far].add(far_back)
    forces = summed.reshape(clusters, 3, 8).transpose(1, 0, 2).reshape(3, atoms_here)
    total = jnp.sum(kinetic)
    volume = box_lengths[0] * box_lengths[1] * box_lengths[2]
    thermal_ratio_value = 2.0 * total / (3.0 * (atoms_here * axis_count) * thermal_scale_unit)
    reservoir_damping = extended_variables[0] + reservoir_inertia_mass * (thermal_ratio_value - 1.0)
    box_rates = extended_variables[1:] + barostat_gain * (
        kinetic - virial_total - pressure_target * volume / 2.0
    ) / (total / 3.0)
    new_velocities = velocities + time_step * (
        forces * inverse_mass[None, :] - (reservoir_damping + box_rates[:, None]) * velocities
    )
    new_positions = positions * (1.0 + time_step * box_rates[:, None]) + time_step * new_velocities
    new_coupling = jnp.concatenate([reservoir_damping[None], box_rates])
    return (forces, new_velocities, new_positions, new_coupling)


def solution(mesh):
    return jax.shard_map(
        on_device,
        mesh=mesh,
        in_specs=(
            P(None, ("rep", "gx")),
            P(None, ("rep", "gx")),
            P(None, ("rep", "gx")),
            P(None, ("rep", "gx")),
            P(("rep", "gx")),
            P(None, ("rep", "gx")),
            P(("rep", "gx")),
            P("rep"),
            P("rep"),
        ),
        out_specs=(
            P(None, ("rep", "gx")),
            P(None, ("rep", "gx")),
            P(None, ("rep", "gx")),
            P("rep"),
        ),
        check_vma=False,
    )
```

```python
import functools

import jax
import jax.numpy as jnp
from jax import lax
from jax.experimental import pallas as pl
from jax.experimental.pallas import tpu as pltpu
from jax.sharding import PartitionSpec as P

time_step = 0.25
reaction_term = 1.0 / 1331.0
thermal_scale_unit = 2.0
reservoir_inertia_mass = 4.0
barostat_gain = 0.1
pressure_target = 1.0

LANES = 128


def round_up(value, unit):
    return (value + unit - 1) // unit * unit


def split_three(value):
    high = value.astype(jnp.bfloat16).astype(jnp.float32)
    rest = value - high
    middle = rest.astype(jnp.bfloat16).astype(jnp.float32)
    return jnp.concatenate([high, middle, rest - middle], axis=0).astype(jnp.bfloat16)


def one_hot_rows(index_row, rows, ramp):
    pieces = []
    for base in range(0, rows, 256):
        height = min(256, rows - base)
        moved = (index_row - base).astype(jnp.float32)
        moved = jnp.broadcast_to(moved, (16, LANES)).astype(jnp.bfloat16)
        for first in range(0, height, 16):
            hit = moved == ramp[first : first + 16]
            pieces.append(jnp.where(hit, jnp.bfloat16(1), jnp.bfloat16(0)))
    return jnp.concatenate(pieces, axis=0)


def gathered(table_ref, index_row, tiles):
    index = jnp.broadcast_to(index_row, (8, LANES))
    within = index & (LANES - 1)
    block = index // LANES
    result = []
    for component in range(6):
        value = None
        for tile in range(tiles):
            source = table_ref[component * 8 : component * 8 + 8, tile * LANES : (tile + 1) * LANES]
            picked = jnp.take_along_axis(source, within, axis=1, mode="promise_in_bounds")
            value = picked if value is None else jnp.where(block == tile, picked, value)
        result.append(value)
    return result


def pair_kernel(
    count_ref, box_ref, lift_ref, here_ref, near_ref, beyond_ref, chosen_ref, velocity_ref,
    param_ref, pair_ref, word_ref, own_ref, other_ref, sum_ref,
    table_ref, wide_ref, virial_ref, first_terms, second_terms, *, clusters, slots, block
):
    sublane = lax.broadcasted_iota(jnp.int32, (8, LANES), 0)
    lane = lax.broadcasted_iota(jnp.int32, (8, LANES), 1)
    ramp = lax.broadcasted_iota(jnp.int32, (256, LANES), 0).astype(jnp.float32).astype(jnp.bfloat16)
    count = count_ref[0]
    box_y = box_ref[1]
    box_z = box_ref[2]
    first_tiles = -(-clusters // LANES)
    second_tiles = -(-slots // LANES)
    near_lift = jnp.where(lift_ref[0] >= 1, box_ref[0], 0.0)
    far_lift = jnp.where(lift_ref[0] >= 0, box_ref[0], 0.0)
    upper = lax.broadcasted_iota(jnp.int32, (48, clusters), 0) < 8
    table_ref[:, slots - slots % LANES :] = jnp.zeros((48, table_ref.shape[1] - slots + slots % LANES), jnp.float32)
    table_ref[:, 0:clusters] = here_ref[...]
    table_ref[:, clusters : 2 * clusters] = near_ref[...] + jnp.where(upper, near_lift, 0.0)
    wide_ref[...] = jnp.zeros_like(wide_ref)
    wide_ref[:, 0:clusters] = beyond_ref[...]
    far_count = slots - 2 * clusters
    for start in range(0, far_count, LANES):
        width = min(LANES, far_count - start)
        values = gathered(wide_ref, chosen_ref[0:1, start : start + LANES], first_tiles)
        values[0] = values[0] + far_lift
        for component in range(6):
            table_ref[
                component * 8 : component * 8 + 8, 2 * clusters + start : 2 * clusters + start + width
            ] = values[component][:, :width]
    own_ref[...] = jnp.zeros_like(own_ref)
    other_ref[...] = jnp.zeros_like(other_ref)
    virial_ref[...] = jnp.zeros_like(virial_ref)

    def one_block(number, carry):
        start = pl.multiple_of(number * block, LANES)
        first_hot = []
        second_hot = []
        virial = [virial_ref[c * 8 : c * 8 + 8, :] for c in range(3)]
        for part in range(block // LANES):
            at = pl.multiple_of(start + part * LANES, LANES)
            here = pl.ds(at, LANES)
            first_row = pair_ref[0:1, here]
            second_row = pair_ref[1:2, here]
            image = jnp.broadcast_to(pair_ref[2:3, here], (8, LANES))
            first = gathered(table_ref, first_row, first_tiles)
            second = gathered(table_ref, second_row, second_tiles)
            step_y = jnp.where(image >= 6, 1.0, jnp.where(image >= 3, 0.0, -1.0))
            step_z = image.astype(jnp.float32) - 3.0 * step_y - 4.0
            shift = (None, step_y * box_y, step_z * box_z)
            for c in range(3):
                origin = jnp.broadcast_to(first[c][0:1], (8, LANES))
                second[c] = second[c] - origin
                if shift[c] is not None:
                    second[c] = second[c] + shift[c]
                first[c] = first[c] - origin
            words = [jnp.broadcast_to(word_ref[w : w + 1, here], (8, LANES)) for w in range(4)]
            low = jnp.where(sublane < 2, words[0], words[1])
            high = jnp.where(sublane < 6, words[2], words[3])
            bits = jnp.where(sublane < 4, low, high) >> (8 * (sublane & 1))
            bits = jnp.where(at + lane < count, bits, 0)
            charge, dispersion, repulsion = first[3], 6.0 * first[4], 12.0 * first[5]
            moving = list(second)
            onto_first = [None] * 3
            onto_second = [None] * 3
            for turn in range(7, -1, -1):
                moving = [pltpu.roll(m, 1, 0) for m in moving] if turn else second
                delta = [moving[c] - first[c] for c in range(3)]
                radius_sq = delta[0] * delta[0] + delta[1] * delta[1] + delta[2] * delta[2]
                inverse = lax.rsqrt(radius_sq)
                inverse_sq = inverse * inverse
                cube = inverse * inverse_sq
                six = cube * cube
                scalar = charge * moving[3] * (cube - reaction_term) + (
                    repulsion * moving[5] * six - dispersion * moving[4]
                ) * (six * inverse_sq)
                wanted = (bits & (1 << ((sublane + turn) & 7))) != 0
                scalar = jnp.where(wanted, scalar, 0.0)
                for c in range(3):
                    force = scalar * delta[c]
                    if onto_first[c] is None:
                        onto_first[c] = -force
                        onto_second[c] = force
                    else:
                        onto_first[c] = onto_first[c] - force
                        onto_second[c] = pltpu.roll(onto_second[c], 1, 0) + force
            for c in range(3):
                virial[c] = virial[c] + (onto_second[c] * second[c] + onto_first[c] * first[c])
            lanes = slice(part * LANES, (part + 1) * LANES)
            first_terms[:, lanes] = split_three(jnp.concatenate(onto_first, axis=0))
            second_terms[:, lanes] = split_three(jnp.concatenate(onto_second, axis=0))
            first_hot.append(one_hot_rows(first_row, clusters, ramp))
            second_hot.append(one_hot_rows(second_row, slots, ramp))
        for c in range(3):
            virial_ref[c * 8 : c * 8 + 8, :] = virial[c]
        contract = (((1,), (1,)), ((), ()))
        own_ref[...] += lax.dot_general(
            jnp.concatenate(first_hot, axis=1), first_terms[...], contract,
            preferred_element_type=jnp.float32,
        )
        other_ref[...] += lax.dot_general(
            jnp.concatenate(second_hot, axis=1), second_terms[...], contract,
            preferred_element_type=jnp.float32,
        )
        return carry

    lax.fori_loop(0, (count + block - 1) // block, one_block, 0)
    energy = velocity_ref[...] * velocity_ref[...] / param_ref[3:4, :]
    energy = 0.5 * jnp.sum(energy, axis=1, keepdims=True)
    rows = [
        jnp.sum(jnp.sum(virial_ref[c * 8 : c * 8 + 8, :], axis=0, keepdims=True), axis=1, keepdims=True) * -0.5
        for c in range(3)
    ]
    rows = rows + [energy, jnp.zeros((2, 1), jnp.float32)]
    sum_ref[...] = jnp.broadcast_to(jnp.concatenate(rows, axis=0), (8, LANES))


def pair_forces(scalars, arrays, pair_list, exclusion, clusters, slots):
    pairs = pair_list.shape[1]
    block = next(b for b in (512, 384, 256, 128) if pairs % b == 0)
    vmem = pl.BlockSpec(memory_space=pltpu.VMEM)
    smem = pl.BlockSpec(memory_space=pltpu.SMEM)
    return pl.pallas_call(
        functools.partial(pair_kernel, clusters=clusters, slots=slots, block=block),
        name="pair_kernel",
        out_shape=(
            jax.ShapeDtypeStruct((clusters, 72), jnp.float32),
            jax.ShapeDtypeStruct((slots, 72), jnp.float32),
            jax.ShapeDtypeStruct((8, LANES), jnp.float32),
        ),
        in_specs=[smem] * 3 + [vmem] * 8,
        out_specs=(vmem, vmem, vmem),
        scratch_shapes=[
            pltpu.VMEM((48, round_up(slots, LANES)), jnp.float32),
            pltpu.VMEM((48, round_up(clusters, LANES)), jnp.float32),
            pltpu.VMEM((24, LANES), jnp.float32),
            pltpu.VMEM((72, block), jnp.bfloat16),
            pltpu.VMEM((72, block), jnp.bfloat16),
        ],
    )(*scalars, *arrays, pair_list, exclusion)


def send(source, target, sems, place, device):
    return pltpu.make_async_remote_copy(
        src_ref=source,
        dst_ref=target,
        send_sem=sems[0].at[place],
        recv_sem=sems[1].at[place],
        device_id={"gx": device},
        device_id_type=pl.DeviceIdType.MESH,
    )


def forward_kernel(packed_ref, chosen_ref, near_ref, beyond_ref, picked_ref, send_sems, recv_sems, *, count):
    me = lax.axis_index("gx")
    barrier = pltpu.get_barrier_semaphore()
    for step in (1, 2, count - 1, count - 2):
        pl.semaphore_signal(
            barrier, inc=1, device_id={"gx": lax.rem(me + step, count)},
            device_id_type=pl.DeviceIdType.MESH,
        )
    pl.semaphore_wait(barrier, 4)
    below = lax.rem(me + count - 1, count)
    far_below = lax.rem(me + count - 2, count)
    sems = (send_sems, recv_sems)
    copies = [
        send(packed_ref, beyond_ref, sems, 1, far_below),
        send(chosen_ref, picked_ref, sems, 2, far_below),
        send(packed_ref, near_ref, sems, 0, below),
    ]
    for copy in copies:
        copy.start()
    for copy in copies:
        copy.wait()


def forward(packed, chosen, count):
    vmem = pl.BlockSpec(memory_space=pltpu.VMEM)
    return pl.pallas_call(
        functools.partial(forward_kernel, count=count),
        name="forward_kernel",
        out_shape=(
            jax.ShapeDtypeStruct(packed.shape, packed.dtype),
            jax.ShapeDtypeStruct(packed.shape, packed.dtype),
            jax.ShapeDtypeStruct(chosen.shape, chosen.dtype),
        ),
        in_specs=[vmem] * 2,
        out_specs=(vmem,) * 3,
        scratch_shapes=[pltpu.SemaphoreType.DMA((3,)), pltpu.SemaphoreType.DMA((3,))],
        compiler_params=pltpu.CompilerParams(collective_id=0, has_side_effects=True),
    )(packed, chosen)


def return_kernel(
    box_ref, extended_ref, near_ref, far_ref, sum_ref, near_back, far_back, rate_ref,
    all_sums, send_sems, recv_sems, give_sems, take_sems, *, count, particles
):
    me = lax.axis_index("gx")
    barrier = pltpu.get_barrier_semaphore()

    def greet(step, carry):
        pl.semaphore_signal(
            barrier, inc=1, device_id={"gx": lax.rem(me + step, count)},
            device_id_type=pl.DeviceIdType.MESH,
        )
        return carry

    lax.fori_loop(1, count, greet, 0)
    pl.semaphore_wait(barrier, count - 1)
    sems = (send_sems, recv_sems)
    copies = [
        send(far_ref, far_back, sems, 1, lax.rem(me + 2, count)),
        send(near_ref, near_back, sems, 0, lax.rem(me + 1, count)),
    ]

    def sum_copy(step, source):
        return pltpu.make_async_remote_copy(
            src_ref=sum_ref,
            dst_ref=all_sums.at[source],
            send_sem=give_sems.at[step],
            recv_sem=take_sems.at[source],
            device_id={"gx": lax.rem(me + step, count)},
            device_id_type=pl.DeviceIdType.MESH,
        )

    def give(step, carry):
        sum_copy(step, me).start()
        return carry

    def take(step, carry):
        sum_copy(step, lax.rem(me + count - step, count)).wait()
        return carry

    lax.fori_loop(1, count, give, 0)
    for copy in copies:
        copy.start()
    all_sums[me] = sum_ref[...]
    lax.fori_loop(1, count, take, 0)
    total = lax.fori_loop(
        0, count, lambda source, held: held + all_sums[source], jnp.zeros((8, LANES), jnp.float32)
    )
    virial = total[0:3]
    kinetic = total[3:6]
    energy = total[3:4] + total[4:5] + total[5:6]
    volume = box_ref[0] * box_ref[1] * box_ref[2]
    ratio = 2.0 * energy / (3.0 * particles * thermal_scale_unit)
    rate_ref[3:4] = extended_ref[0] + reservoir_inertia_mass * (ratio - 1.0)
    change = barostat_gain * (kinetic - virial - pressure_target * volume / 2.0) / (energy / 3.0)
    for c in range(3):
        rate_ref[c : c + 1] = extended_ref[1 + c] + change[c : c + 1]
    for copy in copies:
        copy.wait()


def returned(box_lengths, extended_variables, near, far, sums, count, particles):
    vmem = pl.BlockSpec(memory_space=pltpu.VMEM)
    smem = pl.BlockSpec(memory_space=pltpu.SMEM)
    return pl.pallas_call(
        functools.partial(return_kernel, count=count, particles=particles),
        name="return_kernel",
        out_shape=(
            jax.ShapeDtypeStruct(near.shape, near.dtype),
            jax.ShapeDtypeStruct(far.shape, far.dtype),
            jax.ShapeDtypeStruct((4, LANES), jnp.float32),
        ),
        in_specs=[smem] * 2 + [vmem] * 3,
        out_specs=(vmem,) * 3,
        scratch_shapes=[
            pltpu.VMEM((count, 8, LANES), jnp.float32),
            pltpu.SemaphoreType.DMA((2,)),
            pltpu.SemaphoreType.DMA((2,)),
            pltpu.SemaphoreType.DMA((count,)),
            pltpu.SemaphoreType.DMA((count,)),
        ],
        compiler_params=pltpu.CompilerParams(collective_id=1, has_side_effects=True),
    )(box_lengths, extended_variables, near, far, sums)


def on_device(
    positions,
    velocities,
    atom_params,
    pair_list,
    pair_count,
    exclusion,
    halo_far,
    box_lengths,
    extended_variables,
):
    atoms_here = positions.shape[1]
    clusters = atoms_here // 8
    far_clusters = halo_far.shape[0]
    slots = 2 * clusters + far_clusters
    axis_count = lax.axis_size("gx")
    inverse_mass = atom_params[3]
    packed = jnp.concatenate([positions, atom_params[:3]], axis=0)
    packed = packed.reshape(6, clusters, 8).transpose(0, 2, 1).reshape(48, clusters)
    chosen = jnp.pad(halo_far, (0, round_up(far_clusters, LANES) - far_clusters))[None, :]
    near_rows, beyond, picked = forward(packed, chosen, axis_count)
    lift = (lax.axis_index("gx") - (axis_count - 2)).astype(jnp.int32)[None]
    own, other, sums = pair_forces(
        (pair_count, box_lengths, lift),
        (packed, near_rows, beyond, picked, velocities, atom_params),
        pair_list, exclusion, clusters, slots,
    )
    other = other[:, :24] + other[:, 24:48] + other[:, 48:]
    near_back, far_back, rates = returned(
        box_lengths, extended_variables, other[clusters : 2 * clusters], other[2 * clusters :],
        sums, axis_count, atoms_here * axis_count,
    )
    own = own[:, :24] + own[:, 24:48] + own[:, 48:] + other[:clusters]
    summed = (own + near_back).at[halo_far].add(far_back)
    forces = summed.reshape(clusters, 3, 8).transpose(1, 0, 2).reshape(3, atoms_here)
    box_rates = rates[:3, :1]
    reservoir_damping = rates[3:, :1]
    new_velocities = velocities + time_step * (
        forces * inverse_mass[None, :] - (reservoir_damping + box_rates) * velocities
    )
    new_positions = positions * (1.0 + time_step * box_rates) + time_step * new_velocities
    new_coupling = jnp.concatenate([rates[3:, 0], rates[:3, 0]])
    return (forces, new_velocities, new_positions, new_coupling)


def solution(mesh):
    return jax.shard_map(
        on_device,
        mesh=mesh,
        in_specs=(
            P(None, ("rep", "gx")),
            P(None, ("rep", "gx")),
            P(None, ("rep", "gx")),
            P(None, ("rep", "gx")),
            P(("rep", "gx")),
            P(None, ("rep", "gx")),
            P(("rep", "gx")),
            P("rep"),
            P("rep"),
        ),
        out_specs=(
            P(None, ("rep", "gx")),
            P(None, ("rep", "gx")),
            P(None, ("rep", "gx")),
            P("rep"),
        ),
        check_vma=False,
    )
```

```python
import functools

import jax
import jax.numpy as jnp
from jax import lax
from jax.experimental import pallas as pl
from jax.experimental.pallas import tpu as pltpu
from jax.sharding import PartitionSpec as P

time_step = 0.25
reaction_term = 1.0 / 1331.0
thermal_scale_unit = 2.0
reservoir_inertia_mass = 4.0
barostat_gain = 0.1
pressure_target = 1.0

LANES = 128


def round_up(value, unit):
    return (value + unit - 1) // unit * unit


def split_three(value):
    high = value.astype(jnp.bfloat16).astype(jnp.float32)
    rest = value - high
    middle = rest.astype(jnp.bfloat16).astype(jnp.float32)
    return jnp.concatenate([high, middle, rest - middle], axis=0).astype(jnp.bfloat16)


def one_hot_rows(index_row, rows, ramp):
    pieces = []
    for base in range(0, rows, 256):
        height = min(256, rows - base)
        moved = (index_row - base).astype(jnp.float32)
        moved = jnp.broadcast_to(moved, (16, LANES)).astype(jnp.bfloat16)
        for first in range(0, height, 16):
            hit = moved == ramp[first : first + 16]
            pieces.append(jnp.where(hit, jnp.bfloat16(1), jnp.bfloat16(0)))
    return jnp.concatenate(pieces, axis=0)


def gathered(table_ref, index_row, tiles):
    index = jnp.broadcast_to(index_row, (8, LANES))
    within = index & (LANES - 1)
    block = index // LANES
    result = []
    for component in range(6):
        value = None
        for tile in range(tiles):
            source = table_ref[component * 8 : component * 8 + 8, tile * LANES : (tile + 1) * LANES]
            picked = jnp.take_along_axis(source, within, axis=1, mode="promise_in_bounds")
            value = picked if value is None else jnp.where(block == tile, picked, value)
        result.append(value)
    return result


def pair_kernel(
    count_ref, box_ref, lift_ref, here_ref, near_ref, beyond_ref, chosen_ref, velocity_ref,
    param_ref, pair_ref, word_ref, own_out, near_out, far_out, sum_ref,
    table_ref, wide_ref, virial_ref, first_got, second_got, bits_got, first_terms, second_terms,
    own_ref, other_ref, *, clusters, slots, block
):
    sublane = lax.broadcasted_iota(jnp.int32, (8, LANES), 0)
    lane = lax.broadcasted_iota(jnp.int32, (8, LANES), 1)
    ramp = lax.broadcasted_iota(jnp.int32, (256, LANES), 0).astype(jnp.float32).astype(jnp.bfloat16)
    count = count_ref[0]
    box_y = box_ref[1]
    box_z = box_ref[2]
    first_tiles = -(-clusters // LANES)
    second_tiles = -(-slots // LANES)
    near_lift = jnp.where(lift_ref[0] >= 1, box_ref[0], 0.0)
    far_lift = jnp.where(lift_ref[0] >= 0, box_ref[0], 0.0)
    upper = lax.broadcasted_iota(jnp.int32, (48, clusters), 0) < 8
    tail = slots - slots % LANES
    if tail < table_ref.shape[1]:
        table_ref[:, tail:] = jnp.zeros((48, table_ref.shape[1] - tail), jnp.float32)
    table_ref[:, 0:clusters] = here_ref[...]
    table_ref[:, clusters : 2 * clusters] = near_ref[...] + jnp.where(upper, near_lift, 0.0)
    wide_ref[...] = jnp.zeros_like(wide_ref)
    wide_ref[:, 0:clusters] = beyond_ref[...]
    far_count = slots - 2 * clusters
    for start in range(0, far_count, LANES):
        width = min(LANES, far_count - start)
        values = gathered(wide_ref, chosen_ref[0:1, start : start + LANES], first_tiles)
        values[0] = values[0] + far_lift
        for component in range(6):
            table_ref[
                component * 8 : component * 8 + 8, 2 * clusters + start : 2 * clusters + start + width
            ] = values[component][:, :width]
    own_ref[...] = jnp.zeros_like(own_ref)
    other_ref[...] = jnp.zeros_like(other_ref)
    virial_ref[...] = jnp.zeros_like(virial_ref)
    first_terms[...] = jnp.zeros_like(first_terms)
    second_terms[...] = jnp.zeros_like(second_terms)

    def fetch(number, part):
        at = pl.multiple_of(number * block + part * LANES, LANES)
        here = pl.ds(at, LANES)
        lanes = slice(part * LANES, (part + 1) * LANES)
        image = jnp.broadcast_to(pair_ref[2:3, here], (8, LANES))
        first = gathered(table_ref, pair_ref[0:1, here], first_tiles)
        second = gathered(table_ref, pair_ref[1:2, here], second_tiles)
        step_y = jnp.where(image >= 6, 1.0, jnp.where(image >= 3, 0.0, -1.0))
        step_z = image.astype(jnp.float32) - 3.0 * step_y - 4.0
        shift = (None, step_y * box_y, step_z * box_z)
        for c in range(3):
            origin = jnp.broadcast_to(first[c][0:1], (8, LANES))
            second[c] = second[c] - origin
            if shift[c] is not None:
                second[c] = second[c] + shift[c]
            first[c] = first[c] - origin
        words = [jnp.broadcast_to(word_ref[w : w + 1, here], (8, LANES)) for w in range(4)]
        low = jnp.where(sublane < 2, words[0], words[1])
        high = jnp.where(sublane < 6, words[2], words[3])
        bits = jnp.where(sublane < 4, low, high) >> (8 * (sublane & 1))
        bits_got[:, lanes] = jnp.where(at + lane < count, bits, 0)
        first[4] = 6.0 * first[4]
        first[5] = 12.0 * first[5]
        for c in range(6):
            first_got[c * 8 : c * 8 + 8, lanes] = first[c]
            second_got[c * 8 : c * 8 + 8, lanes] = second[c]

    def interact(part):
        lanes = slice(part * LANES, (part + 1) * LANES)
        first = [first_got[c * 8 : c * 8 + 8, lanes] for c in range(6)]
        second = [second_got[c * 8 : c * 8 + 8, lanes] for c in range(6)]
        bits = bits_got[:, lanes]
        charge, dispersion, repulsion = first[3], first[4], first[5]
        moving = second
        onto_first = [None] * 3
        onto_second = [None] * 3
        for turn in range(7, -1, -1):
            moving = [pltpu.roll(m, 1, 0) for m in moving] if turn else second
            delta = [moving[c] - first[c] for c in range(3)]
            radius_sq = delta[0] * delta[0] + delta[1] * delta[1] + delta[2] * delta[2]
            inverse = lax.rsqrt(radius_sq)
            inverse_sq = inverse * inverse
            cube = inverse * inverse_sq
            six = cube * cube
            scalar = charge * moving[3] * (cube - reaction_term) + (
                repulsion * moving[5] * six - dispersion * moving[4]
            ) * (six * inverse_sq)
            wanted = (bits & (1 << ((sublane + turn) & 7))) != 0
            scalar = jnp.where(wanted, scalar, 0.0)
            for c in range(3):
                force = scalar * delta[c]
                if onto_first[c] is None:
                    onto_first[c] = -force
                    onto_second[c] = force
                else:
                    onto_first[c] = onto_first[c] - force
                    onto_second[c] = pltpu.roll(onto_second[c], 1, 0) + force
        first_terms[:, lanes] = split_three(jnp.concatenate(onto_first, axis=0))
        second_terms[:, lanes] = split_three(jnp.concatenate(onto_second, axis=0))
        return [onto_second[c] * second[c] + onto_first[c] * first[c] for c in range(3)]

    def spread(number):
        first_hot = []
        second_hot = []
        for part in range(block // LANES):
            here = pl.ds(pl.multiple_of(number * block + part * LANES, LANES), LANES)
            first_hot.append(one_hot_rows(pair_ref[0:1, here], clusters, ramp))
            second_hot.append(one_hot_rows(pair_ref[1:2, here], slots, ramp))
        contract = (((1,), (1,)), ((), ()))
        own_ref[...] += lax.dot_general(
            first_terms[...], jnp.concatenate(first_hot, axis=1), contract,
            preferred_element_type=jnp.float32,
        )
        other_ref[...] += lax.dot_general(
            second_terms[...], jnp.concatenate(second_hot, axis=1), contract,
            preferred_element_type=jnp.float32,
        )

    blocks = jnp.maximum((count + block - 1) // block, 1)
    for part in range(block // LANES):
        fetch(0, part)

    def one_block(number, carry):
        spread(jnp.maximum(number - 1, 0))
        upcoming = jnp.minimum(number + 1, blocks - 1)
        virial = [virial_ref[c * 8 : c * 8 + 8, :] for c in range(3)]
        for part in range(block // LANES):
            added = interact(part)
            virial = [virial[c] + added[c] for c in range(3)]
            fetch(upcoming, part)
        for c in range(3):
            virial_ref[c * 8 : c * 8 + 8, :] = virial[c]
        return carry

    lax.fori_loop(0, blocks, one_block, 0)
    spread(blocks - 1)
    other = other_ref[0:24, :] + other_ref[24:48, :] + other_ref[48:72, :]
    own_out[...] = own_ref[0:24, :] + own_ref[24:48, :] + own_ref[48:72, :] + other[:, 0:clusters]
    near_out[...] = other[:, clusters : 2 * clusters]
    far_sum = jnp.zeros((72, clusters), jnp.float32)
    for start in range(0, far_count, LANES):
        width = min(LANES, far_count - start)
        piece = other[:, 2 * clusters + start : 2 * clusters + start + width]
        if width < LANES:
            piece = jnp.concatenate([piece, jnp.zeros((24, LANES - width), jnp.float32)], axis=1)
        far_sum = far_sum + lax.dot_general(
            split_three(piece),
            one_hot_rows(chosen_ref[0:1, start : start + LANES], clusters, ramp),
            (((1,), (1,)), ((), ())), preferred_element_type=jnp.float32,
        )
    far_out[...] = far_sum[0:24] + far_sum[24:48] + far_sum[48:72]
    energy = velocity_ref[...] * velocity_ref[...] / param_ref[3:4, :]
    energy = 0.5 * jnp.sum(energy, axis=1, keepdims=True)
    rows = [
        jnp.sum(jnp.sum(virial_ref[c * 8 : c * 8 + 8, :], axis=0, keepdims=True), axis=1, keepdims=True) * -0.5
        for c in range(3)
    ]
    rows = rows + [energy, jnp.zeros((2, 1), jnp.float32)]
    sum_ref[...] = jnp.broadcast_to(jnp.concatenate(rows, axis=0), (8, LANES))


def pair_forces(scalars, arrays, pair_list, exclusion, clusters, slots):
    pairs = pair_list.shape[1]
    block = next(b for b in (512, 384, 256, 128) if pairs % b == 0)
    vmem = pl.BlockSpec(memory_space=pltpu.VMEM)
    smem = pl.BlockSpec(memory_space=pltpu.SMEM)
    folded = jax.ShapeDtypeStruct((24, clusters), jnp.float32)
    return pl.pallas_call(
        functools.partial(pair_kernel, clusters=clusters, slots=slots, block=block),
        name="pair_kernel",
        out_shape=(folded, folded, folded, jax.ShapeDtypeStruct((8, LANES), jnp.float32)),
        in_specs=[smem] * 3 + [vmem] * 8,
        out_specs=(vmem,) * 4,
        scratch_shapes=[
            pltpu.VMEM((48, round_up(slots, LANES)), jnp.float32),
            pltpu.VMEM((48, round_up(clusters, LANES)), jnp.float32),
            pltpu.VMEM((24, LANES), jnp.float32),
            pltpu.VMEM((48, block), jnp.float32),
            pltpu.VMEM((48, block), jnp.float32),
            pltpu.VMEM((8, block), jnp.int32),
            pltpu.VMEM((72, block), jnp.bfloat16),
            pltpu.VMEM((72, block), jnp.bfloat16),
            pltpu.VMEM((72, clusters), jnp.float32),
            pltpu.VMEM((72, slots), jnp.float32),
        ],
    )(*scalars, *arrays, pair_list, exclusion)


def final_kernel(
    own_ref, near_ref, far_ref, rate_ref, position_ref, velocity_ref, param_ref,
    force_out, velocity_out, position_out, folded_ref, *, clusters
):
    sublane = lax.broadcasted_iota(jnp.int32, (8, LANES), 0)
    lane = lax.broadcasted_iota(jnp.int32, (8, LANES), 1)
    wanted = sublane == (lane & 7)
    folded_ref[...] = jnp.zeros_like(folded_ref)
    folded_ref[:, 0:clusters] = own_ref[...] + near_ref[...] + far_ref[...]
    for c in range(3):
        for tile in range(clusters * 8 // LANES):
            at = tile * 16
            source = folded_ref[c * 8 : c * 8 + 8, at // LANES * LANES : at // LANES * LANES + LANES]
            picked = jnp.take_along_axis(
                source, at % LANES + lane // 8, axis=1, mode="promise_in_bounds"
            )
            force_out[c : c + 1, tile * LANES : (tile + 1) * LANES] = jnp.sum(
                jnp.where(wanted, picked, 0.0), axis=0, keepdims=True
            )
    rates = rate_ref[0:3, 0:1]
    damping = rate_ref[3:4, 0:1]
    velocity = velocity_ref[...]
    moved = velocity + time_step * (
        force_out[...] * param_ref[3:4, :] - (damping + rates) * velocity
    )
    velocity_out[...] = moved
    position_out[...] = position_ref[...] * (1.0 + time_step * rates) + time_step * moved


def finished(own, near_back, far_back, rates, positions, velocities, atom_params):
    vmem = pl.BlockSpec(memory_space=pltpu.VMEM)
    clusters = own.shape[1]
    shape = jax.ShapeDtypeStruct(positions.shape, jnp.float32)
    return pl.pallas_call(
        functools.partial(final_kernel, clusters=clusters),
        name="final_kernel",
        out_shape=(shape,) * 3,
        in_specs=[vmem] * 7,
        out_specs=(vmem,) * 3,
        scratch_shapes=[pltpu.VMEM((24, round_up(clusters, LANES)), jnp.float32)],
    )(own, near_back, far_back, rates, positions, velocities, atom_params)


def send(source, target, sems, place, device):
    return pltpu.make_async_remote_copy(
        src_ref=source,
        dst_ref=target,
        send_sem=sems[0].at[place],
        recv_sem=sems[1].at[place],
        device_id={"gx": device},
        device_id_type=pl.DeviceIdType.MESH,
    )


def forward_kernel(packed_ref, chosen_ref, near_ref, beyond_ref, picked_ref, send_sems, recv_sems, *, count):
    me = lax.axis_index("gx")
    barrier = pltpu.get_barrier_semaphore()
    for step in (1, 2, count - 1, count - 2):
        pl.semaphore_signal(
            barrier, inc=1, device_id={"gx": lax.rem(me + step, count)},
            device_id_type=pl.DeviceIdType.MESH,
        )
    pl.semaphore_wait(barrier, 4)
    below = lax.rem(me + count - 1, count)
    far_below = lax.rem(me + count - 2, count)
    sems = (send_sems, recv_sems)
    copies = [
        send(packed_ref, beyond_ref, sems, 1, far_below),
        send(chosen_ref, picked_ref, sems, 2, far_below),
        send(packed_ref, near_ref, sems, 0, below),
    ]
    for copy in copies:
        copy.start()
    for copy in copies:
        copy.wait()


def forward(packed, chosen, count):
    vmem = pl.BlockSpec(memory_space=pltpu.VMEM)
    return pl.pallas_call(
        functools.partial(forward_kernel, count=count),
        name="forward_kernel",
        out_shape=(
            jax.ShapeDtypeStruct(packed.shape, packed.dtype),
            jax.ShapeDtypeStruct(packed.shape, packed.dtype),
            jax.ShapeDtypeStruct(chosen.shape, chosen.dtype),
        ),
        in_specs=[vmem] * 2,
        out_specs=(vmem,) * 3,
        scratch_shapes=[pltpu.SemaphoreType.DMA((3,)), pltpu.SemaphoreType.DMA((3,))],
        compiler_params=pltpu.CompilerParams(collective_id=0, has_side_effects=True),
    )(packed, chosen)


def return_kernel(
    box_ref, extended_ref, near_ref, far_ref, sum_ref, near_back, far_back, rate_ref,
    all_sums, send_sems, recv_sems, give_sems, take_sems, *, count, particles
):
    me = lax.axis_index("gx")
    barrier = pltpu.get_barrier_semaphore()

    def greet(step, carry):
        pl.semaphore_signal(
            barrier, inc=1, device_id={"gx": lax.rem(me + step, count)},
            device_id_type=pl.DeviceIdType.MESH,
        )
        return carry

    lax.fori_loop(1, count, greet, 0)
    pl.semaphore_wait(barrier, count - 1)
    sems = (send_sems, recv_sems)
    copies = [
        send(far_ref, far_back, sems, 1, lax.rem(me + 2, count)),
        send(near_ref, near_back, sems, 0, lax.rem(me + 1, count)),
    ]

    def sum_copy(step, source):
        return pltpu.make_async_remote_copy(
            src_ref=sum_ref,
            dst_ref=all_sums.at[source],
            send_sem=give_sems.at[step],
            recv_sem=take_sems.at[source],
            device_id={"gx": lax.rem(me + step, count)},
            device_id_type=pl.DeviceIdType.MESH,
        )

    def give(step, carry):
        sum_copy(step, me).start()
        return carry

    def take(step, carry):
        sum_copy(step, lax.rem(me + count - step, count)).wait()
        return carry

    lax.fori_loop(1, count, give, 0)
    for copy in copies:
        copy.start()
    all_sums[me] = sum_ref[...]
    lax.fori_loop(1, count, take, 0)
    total = lax.fori_loop(
        0, count, lambda source, held: held + all_sums[source], jnp.zeros((8, LANES), jnp.float32)
    )
    virial = total[0:3]
    kinetic = total[3:6]
    energy = total[3:4] + total[4:5] + total[5:6]
    volume = box_ref[0] * box_ref[1] * box_ref[2]
    ratio = 2.0 * energy / (3.0 * particles * thermal_scale_unit)
    rate_ref[3:4] = extended_ref[0] + reservoir_inertia_mass * (ratio - 1.0)
    change = barostat_gain * (kinetic - virial - pressure_target * volume / 2.0) / (energy / 3.0)
    for c in range(3):
        rate_ref[c : c + 1] = extended_ref[1 + c] + change[c : c + 1]
    for copy in copies:
        copy.wait()


def returned(box_lengths, extended_variables, near, far, sums, count, particles):
    vmem = pl.BlockSpec(memory_space=pltpu.VMEM)
    smem = pl.BlockSpec(memory_space=pltpu.SMEM)
    return pl.pallas_call(
        functools.partial(return_kernel, count=count, particles=particles),
        name="return_kernel",
        out_shape=(
            jax.ShapeDtypeStruct(near.shape, near.dtype),
            jax.ShapeDtypeStruct(far.shape, far.dtype),
            jax.ShapeDtypeStruct((4, LANES), jnp.float32),
        ),
        in_specs=[smem] * 2 + [vmem] * 3,
        out_specs=(vmem,) * 3,
        scratch_shapes=[
            pltpu.VMEM((count, 8, LANES), jnp.float32),
            pltpu.SemaphoreType.DMA((2,)),
            pltpu.SemaphoreType.DMA((2,)),
            pltpu.SemaphoreType.DMA((count,)),
            pltpu.SemaphoreType.DMA((count,)),
        ],
        compiler_params=pltpu.CompilerParams(collective_id=1, has_side_effects=True),
    )(box_lengths, extended_variables, near, far, sums)


def on_device(
    positions,
    velocities,
    atom_params,
    pair_list,
    pair_count,
    exclusion,
    halo_far,
    box_lengths,
    extended_variables,
):
    atoms_here = positions.shape[1]
    clusters = atoms_here // 8
    far_clusters = halo_far.shape[0]
    slots = 2 * clusters + far_clusters
    axis_count = lax.axis_size("gx")
    packed = jnp.concatenate([positions, atom_params[:3]], axis=0)
    packed = packed.reshape(6, clusters, 8).transpose(0, 2, 1).reshape(48, clusters)
    chosen = jnp.pad(halo_far, (0, round_up(far_clusters, LANES) - far_clusters))[None, :]
    near_rows, beyond, picked = forward(packed, chosen, axis_count)
    lift = (lax.axis_index("gx") - (axis_count - 2)).astype(jnp.int32)[None]
    own, near, far, sums = pair_forces(
        (pair_count, box_lengths, lift),
        (packed, near_rows, beyond, picked, velocities, atom_params),
        pair_list, exclusion, clusters, slots,
    )
    near_back, far_back, rates = returned(
        box_lengths, extended_variables, near, far, sums, axis_count, atoms_here * axis_count
    )
    forces, new_velocities, new_positions = finished(
        own, near_back, far_back, rates, positions, velocities, atom_params
    )
    new_coupling = jnp.concatenate([rates[3:, 0], rates[:3, 0]])
    return (forces, new_velocities, new_positions, new_coupling)


def solution(mesh):
    return jax.shard_map(
        on_device,
        mesh=mesh,
        in_specs=(
            P(None, ("rep", "gx")),
            P(None, ("rep", "gx")),
            P(None, ("rep", "gx")),
            P(None, ("rep", "gx")),
            P(("rep", "gx")),
            P(None, ("rep", "gx")),
            P(("rep", "gx")),
            P("rep"),
            P("rep"),
        ),
        out_specs=(
            P(None, ("rep", "gx")),
            P(None, ("rep", "gx")),
            P(None, ("rep", "gx")),
            P("rep"),
        ),
        check_vma=False,
    )
```

```python
import functools

import jax
import jax.numpy as jnp
from jax import lax
from jax.experimental import pallas as pl
from jax.experimental.pallas import tpu as pltpu
from jax.sharding import PartitionSpec as P

time_step = 0.25
reaction_term = 1.0 / 1331.0
thermal_scale_unit = 2.0
reservoir_inertia_mass = 4.0
barostat_gain = 0.1
pressure_target = 1.0

LANES = 128


def round_up(value, unit):
    return (value + unit - 1) // unit * unit


def split_three(value):
    high = value.astype(jnp.bfloat16).astype(jnp.float32)
    rest = value - high
    middle = rest.astype(jnp.bfloat16).astype(jnp.float32)
    return jnp.concatenate([high, middle, rest - middle], axis=0).astype(jnp.bfloat16)


def one_hot_rows(index_row, rows, ramp):
    pieces = []
    for base in range(0, rows, 256):
        height = min(256, rows - base)
        moved = (index_row - base).astype(jnp.float32)
        moved = jnp.broadcast_to(moved, (16, LANES)).astype(jnp.bfloat16)
        for first in range(0, height, 16):
            hit = moved == ramp[first : first + 16]
            pieces.append(jnp.where(hit, jnp.bfloat16(1), jnp.bfloat16(0)))
    return jnp.concatenate(pieces, axis=0)


def gathered(table_ref, index_row, tiles):
    index = jnp.broadcast_to(index_row, (8, LANES))
    within = index & (LANES - 1)
    block = index // LANES
    result = []
    for component in range(6):
        value = None
        for tile in range(tiles):
            source = table_ref[component * 8 : component * 8 + 8, tile * LANES : (tile + 1) * LANES]
            picked = jnp.take_along_axis(source, within, axis=1, mode="promise_in_bounds")
            value = picked if value is None else jnp.where(block == tile, picked, value)
        result.append(value)
    return result


def pair_kernel(
    count_ref, box_ref, lift_ref, here_ref, near_ref, beyond_ref, chosen_ref, velocity_ref,
    param_ref, pair_ref, word_ref, own_out, near_out, far_out, sum_ref,
    table_ref, wide_ref, virial_ref, first_got, second_got, bits_got, first_terms, second_terms,
    own_ref, other_ref, *, clusters, slots, block
):
    sublane = lax.broadcasted_iota(jnp.int32, (8, LANES), 0)
    lane = lax.broadcasted_iota(jnp.int32, (8, LANES), 1)
    ramp = lax.broadcasted_iota(jnp.int32, (256, LANES), 0).astype(jnp.float32).astype(jnp.bfloat16)
    count = count_ref[0]
    box_y = box_ref[1]
    box_z = box_ref[2]
    first_tiles = -(-clusters // LANES)
    second_tiles = -(-slots // LANES)
    near_lift = jnp.where(lift_ref[0] >= 1, box_ref[0], 0.0)
    far_lift = jnp.where(lift_ref[0] >= 0, box_ref[0], 0.0)
    upper = lax.broadcasted_iota(jnp.int32, (48, clusters), 0) < 8
    tail = slots - slots % LANES
    if tail < table_ref.shape[1]:
        table_ref[:, tail:] = jnp.zeros((48, table_ref.shape[1] - tail), jnp.float32)
    table_ref[:, 0:clusters] = here_ref[...]
    table_ref[:, clusters : 2 * clusters] = near_ref[...] + jnp.where(upper, near_lift, 0.0)
    wide_ref[...] = jnp.zeros_like(wide_ref)
    wide_ref[:, 0:clusters] = beyond_ref[...]
    far_count = slots - 2 * clusters
    for start in range(0, far_count, LANES):
        width = min(LANES, far_count - start)
        values = gathered(wide_ref, chosen_ref[0:1, start : start + LANES], first_tiles)
        values[0] = values[0] + far_lift
        for component in range(6):
            table_ref[
                component * 8 : component * 8 + 8, 2 * clusters + start : 2 * clusters + start + width
            ] = values[component][:, :width]
    own_ref[...] = jnp.zeros_like(own_ref)
    other_ref[...] = jnp.zeros_like(other_ref)
    virial_ref[...] = jnp.zeros_like(virial_ref)
    first_terms[...] = jnp.zeros_like(first_terms)
    second_terms[...] = jnp.zeros_like(second_terms)

    def fetch(number, part):
        at = pl.multiple_of(number * block + part * LANES, LANES)
        here = pl.ds(at, LANES)
        lanes = slice(part * LANES, (part + 1) * LANES)
        image = jnp.broadcast_to(pair_ref[2:3, here], (8, LANES))
        first = gathered(table_ref, pair_ref[0:1, here], first_tiles)
        second = gathered(table_ref, pair_ref[1:2, here], second_tiles)
        step_y = jnp.where(image >= 6, 1.0, jnp.where(image >= 3, 0.0, -1.0))
        step_z = image.astype(jnp.float32) - 3.0 * step_y - 4.0
        shift = (None, step_y * box_y, step_z * box_z)
        for c in range(3):
            origin = jnp.broadcast_to(first[c][0:1], (8, LANES))
            second[c] = second[c] - origin
            if shift[c] is not None:
                second[c] = second[c] + shift[c]
            first[c] = first[c] - origin
        words = [jnp.broadcast_to(word_ref[w : w + 1, here], (8, LANES)) for w in range(4)]
        low = jnp.where(sublane < 2, words[0], words[1])
        high = jnp.where(sublane < 6, words[2], words[3])
        bits = jnp.where(sublane < 4, low, high) >> (8 * (sublane & 1))
        bits_got[:, lanes] = jnp.where(at + lane < count, bits, 0)
        first[4] = 6.0 * first[4]
        first[5] = 12.0 * first[5]
        for c in range(6):
            first_got[c * 8 : c * 8 + 8, lanes] = first[c]
            second_got[c * 8 : c * 8 + 8, lanes] = second[c]

    def interact(part):
        lanes = slice(part * LANES, (part + 1) * LANES)
        first = [first_got[c * 8 : c * 8 + 8, lanes] for c in range(6)]
        second = [second_got[c * 8 : c * 8 + 8, lanes] for c in range(6)]
        bits = bits_got[:, lanes]
        charge, dispersion, repulsion = first[3], first[4], first[5]
        moving = second
        onto_first = [None] * 3
        onto_second = [None] * 3
        for turn in range(7, -1, -1):
            moving = [pltpu.roll(m, 1, 0) for m in moving] if turn else second
            delta = [moving[c] - first[c] for c in range(3)]
            radius_sq = delta[0] * delta[0] + delta[1] * delta[1] + delta[2] * delta[2]
            inverse = lax.rsqrt(radius_sq)
            inverse_sq = inverse * inverse
            cube = inverse * inverse_sq
            six = cube * cube
            scalar = charge * moving[3] * (cube - reaction_term) + (
                repulsion * moving[5] * six - dispersion * moving[4]
            ) * (six * inverse_sq)
            wanted = (bits & (1 << ((sublane + turn) & 7))) != 0
            scalar = jnp.where(wanted, scalar, 0.0)
            for c in range(3):
                force = scalar * delta[c]
                if onto_first[c] is None:
                    onto_first[c] = -force
                    onto_second[c] = force
                else:
                    onto_first[c] = onto_first[c] - force
                    onto_second[c] = pltpu.roll(onto_second[c], 1, 0) + force
        first_terms[:, lanes] = split_three(jnp.concatenate(onto_first, axis=0))
        second_terms[:, lanes] = split_three(jnp.concatenate(onto_second, axis=0))
        return [onto_second[c] * second[c] + onto_first[c] * first[c] for c in range(3)]

    def spread(number):
        first_hot = []
        second_hot = []
        for part in range(block // LANES):
            here = pl.ds(pl.multiple_of(number * block + part * LANES, LANES), LANES)
            first_hot.append(one_hot_rows(pair_ref[0:1, here], clusters, ramp))
            second_hot.append(one_hot_rows(pair_ref[1:2, here], slots, ramp))
        contract = (((1,), (1,)), ((), ()))
        own_ref[...] += lax.dot_general(
            first_terms[...], jnp.concatenate(first_hot, axis=1), contract,
            preferred_element_type=jnp.float32,
        )
        other_ref[...] += lax.dot_general(
            second_terms[...], jnp.concatenate(second_hot, axis=1), contract,
            preferred_element_type=jnp.float32,
        )

    blocks = jnp.maximum((count + block - 1) // block, 1)
    for part in range(block // LANES):
        fetch(0, part)

    def one_block(number, carry):
        spread(jnp.maximum(number - 1, 0))
        upcoming = jnp.minimum(number + 1, blocks - 1)
        virial = [virial_ref[c * 8 : c * 8 + 8, :] for c in range(3)]
        for part in range(block // LANES):
            added = interact(part)
            virial = [virial[c] + added[c] for c in range(3)]
            fetch(upcoming, part)
        for c in range(3):
            virial_ref[c * 8 : c * 8 + 8, :] = virial[c]
        return carry

    lax.fori_loop(0, blocks, one_block, 0)
    spread(blocks - 1)
    other = other_ref[0:24, :] + other_ref[24:48, :] + other_ref[48:72, :]
    own_out[...] = own_ref[0:24, :] + own_ref[24:48, :] + own_ref[48:72, :] + other[:, 0:clusters]
    near_out[...] = other[:, clusters : 2 * clusters]
    far_sum = jnp.zeros((72, clusters), jnp.float32)
    for start in range(0, far_count, LANES):
        width = min(LANES, far_count - start)
        piece = other[:, 2 * clusters + start : 2 * clusters + start + width]
        if width < LANES:
            piece = jnp.concatenate([piece, jnp.zeros((24, LANES - width), jnp.float32)], axis=1)
        far_sum = far_sum + lax.dot_general(
            split_three(piece),
            one_hot_rows(chosen_ref[0:1, start : start + LANES], clusters, ramp),
            (((1,), (1,)), ((), ())), preferred_element_type=jnp.float32,
        )
    far_out[...] = far_sum[0:24] + far_sum[24:48] + far_sum[48:72]
    energy = velocity_ref[...] * velocity_ref[...] / param_ref[3:4, :]
    energy = 0.5 * jnp.sum(energy, axis=1, keepdims=True)
    rows = [
        jnp.sum(jnp.sum(virial_ref[c * 8 : c * 8 + 8, :], axis=0, keepdims=True), axis=1, keepdims=True) * -0.5
        for c in range(3)
    ]
    rows = rows + [energy, jnp.zeros((2, 1), jnp.float32)]
    sum_ref[...] = jnp.broadcast_to(jnp.concatenate(rows, axis=0), (8, LANES))


def pair_forces(scalars, arrays, pair_list, exclusion, clusters, slots):
    pairs = pair_list.shape[1]
    block = next(b for b in (512, 384, 256, 128) if pairs % b == 0)
    vmem = pl.BlockSpec(memory_space=pltpu.VMEM)
    smem = pl.BlockSpec(memory_space=pltpu.SMEM)
    folded = jax.ShapeDtypeStruct((24, clusters), jnp.float32)
    return pl.pallas_call(
        functools.partial(pair_kernel, clusters=clusters, slots=slots, block=block),
        name="pair_kernel",
        out_shape=(folded, folded, folded, jax.ShapeDtypeStruct((8, LANES), jnp.float32)),
        in_specs=[smem] * 3 + [vmem] * 8,
        out_specs=(vmem,) * 4,
        scratch_shapes=[
            pltpu.VMEM((48, round_up(slots, LANES)), jnp.float32),
            pltpu.VMEM((48, round_up(clusters, LANES)), jnp.float32),
            pltpu.VMEM((24, LANES), jnp.float32),
            pltpu.VMEM((48, block), jnp.float32),
            pltpu.VMEM((48, block), jnp.float32),
            pltpu.VMEM((8, block), jnp.int32),
            pltpu.VMEM((72, block), jnp.bfloat16),
            pltpu.VMEM((72, block), jnp.bfloat16),
            pltpu.VMEM((72, clusters), jnp.float32),
            pltpu.VMEM((72, slots), jnp.float32),
        ],
    )(*scalars, *arrays, pair_list, exclusion)


def final_kernel(
    own_ref, near_ref, far_ref, rate_ref, position_ref, velocity_ref, param_ref,
    force_out, velocity_out, position_out, coupling_out, folded_ref, *, clusters
):
    sublane = lax.broadcasted_iota(jnp.int32, (8, LANES), 0)
    lane = lax.broadcasted_iota(jnp.int32, (8, LANES), 1)
    wanted = sublane == (lane & 7)
    folded_ref[...] = jnp.zeros_like(folded_ref)
    folded_ref[:, 0:clusters] = own_ref[...] + near_ref[...] + far_ref[...]
    for c in range(3):
        for tile in range(clusters * 8 // LANES):
            at = tile * 16
            source = folded_ref[c * 8 : c * 8 + 8, at // LANES * LANES : at // LANES * LANES + LANES]
            picked = jnp.take_along_axis(
                source, at % LANES + lane // 8, axis=1, mode="promise_in_bounds"
            )
            force_out[c : c + 1, tile * LANES : (tile + 1) * LANES] = jnp.sum(
                jnp.where(wanted, picked, 0.0), axis=0, keepdims=True
            )
    row = jnp.broadcast_to(rate_ref[3:4, :], (1, LANES))
    for c in range(3):
        row = jnp.where(lane[0:1] == c + 1, rate_ref[c : c + 1, :], row)
    coupling_out[...] = row[:, 0:4]
    rates = rate_ref[0:3, 0:1]
    damping = rate_ref[3:4, 0:1]
    velocity = velocity_ref[...]
    moved = velocity + time_step * (
        force_out[...] * param_ref[3:4, :] - (damping + rates) * velocity
    )
    velocity_out[...] = moved
    position_out[...] = position_ref[...] * (1.0 + time_step * rates) + time_step * moved


def finished(own, near_back, far_back, rates, positions, velocities, atom_params):
    vmem = pl.BlockSpec(memory_space=pltpu.VMEM)
    clusters = own.shape[1]
    shape = jax.ShapeDtypeStruct(positions.shape, jnp.float32)
    return pl.pallas_call(
        functools.partial(final_kernel, clusters=clusters),
        name="final_kernel",
        out_shape=(shape,) * 3 + (jax.ShapeDtypeStruct((1, 4), jnp.float32),),
        in_specs=[vmem] * 7,
        out_specs=(vmem,) * 4,
        scratch_shapes=[pltpu.VMEM((24, round_up(clusters, LANES)), jnp.float32)],
    )(own, near_back, far_back, rates, positions, velocities, atom_params)


def pack_kernel(position_ref, param_ref, halo_ref, packed_out, chosen_out, *, clusters, far):
    sublane = lax.broadcasted_iota(jnp.int32, (8, LANES), 0)
    lane = lax.broadcasted_iota(jnp.int32, (8, LANES), 1)
    place = (lane & 15) * 8 + sublane
    for component in range(6):
        source = position_ref if component < 3 else param_ref
        row = component % 3
        for start in range(0, clusters, LANES):
            width = min(LANES, clusters - start)
            value = jnp.zeros((8, LANES), jnp.float32)
            for piece in range(width // 16):
                at = start * 8 + piece * LANES
                spread = jnp.broadcast_to(source[row : row + 1, at : at + LANES], (8, LANES))
                picked = jnp.take_along_axis(spread, place, axis=1, mode="promise_in_bounds")
                value = jnp.where(lane // 16 == piece, picked, value)
            packed_out[component * 8 : component * 8 + 8, start : start + width] = value[:, :width]
    chosen_out[...] = jnp.zeros_like(chosen_out)
    chosen_out[:, 0:far] = halo_ref[...]


def pack(positions, atom_params, halo_far):
    vmem = pl.BlockSpec(memory_space=pltpu.VMEM)
    clusters = positions.shape[1] // 8
    far = halo_far.shape[0]
    return pl.pallas_call(
        functools.partial(pack_kernel, clusters=clusters, far=far),
        name="pack_kernel",
        out_shape=(
            jax.ShapeDtypeStruct((48, clusters), jnp.float32),
            jax.ShapeDtypeStruct((1, round_up(far, LANES)), jnp.int32),
        ),
        in_specs=[vmem] * 3,
        out_specs=(vmem,) * 2,
    )(positions, atom_params, halo_far[None, :])


def send(source, target, sems, place, device):
    return pltpu.make_async_remote_copy(
        src_ref=source,
        dst_ref=target,
        send_sem=sems[0].at[place],
        recv_sem=sems[1].at[place],
        device_id={"gx": device},
        device_id_type=pl.DeviceIdType.MESH,
    )


def forward_kernel(packed_ref, chosen_ref, near_ref, beyond_ref, picked_ref, send_sems, recv_sems, *, count):
    me = lax.axis_index("gx")
    barrier = pltpu.get_barrier_semaphore()
    for step in (1, 2, count - 1, count - 2):
        pl.semaphore_signal(
            barrier, inc=1, device_id={"gx": lax.rem(me + step, count)},
            device_id_type=pl.DeviceIdType.MESH,
        )
    pl.semaphore_wait(barrier, 4)
    below = lax.rem(me + count - 1, count)
    far_below = lax.rem(me + count - 2, count)
    sems = (send_sems, recv_sems)
    copies = [
        send(packed_ref, beyond_ref, sems, 1, far_below),
        send(chosen_ref, picked_ref, sems, 2, far_below),
        send(packed_ref, near_ref, sems, 0, below),
    ]
    for copy in copies:
        copy.start()
    for copy in copies:
        copy.wait()


def forward(packed, chosen, count):
    vmem = pl.BlockSpec(memory_space=pltpu.VMEM)
    return pl.pallas_call(
        functools.partial(forward_kernel, count=count),
        name="forward_kernel",
        out_shape=(
            jax.ShapeDtypeStruct(packed.shape, packed.dtype),
            jax.ShapeDtypeStruct(packed.shape, packed.dtype),
            jax.ShapeDtypeStruct(chosen.shape, chosen.dtype),
        ),
        in_specs=[vmem] * 2,
        out_specs=(vmem,) * 3,
        scratch_shapes=[pltpu.SemaphoreType.DMA((3,)), pltpu.SemaphoreType.DMA((3,))],
        compiler_params=pltpu.CompilerParams(collective_id=0, has_side_effects=True),
    )(packed, chosen)


def return_kernel(
    box_ref, extended_ref, near_ref, far_ref, sum_ref, near_back, far_back, rate_ref,
    all_sums, send_sems, recv_sems, give_sems, take_sems, *, count, particles
):
    me = lax.axis_index("gx")
    barrier = pltpu.get_barrier_semaphore()

    def greet(step, carry):
        pl.semaphore_signal(
            barrier, inc=1, device_id={"gx": lax.rem(me + step, count)},
            device_id_type=pl.DeviceIdType.MESH,
        )
        return carry

    lax.fori_loop(1, count, greet, 0)
    pl.semaphore_wait(barrier, count - 1)
    sems = (send_sems, recv_sems)
    copies = [
        send(far_ref, far_back, sems, 1, lax.rem(me + 2, count)),
        send(near_ref, near_back, sems, 0, lax.rem(me + 1, count)),
    ]

    def sum_copy(step, source):
        return pltpu.make_async_remote_copy(
            src_ref=sum_ref,
            dst_ref=all_sums.at[source],
            send_sem=give_sems.at[step],
            recv_sem=take_sems.at[source],
            device_id={"gx": lax.rem(me + step, count)},
            device_id_type=pl.DeviceIdType.MESH,
        )

    def give(step, carry):
        sum_copy(step, me).start()
        return carry

    def take(step, carry):
        sum_copy(step, lax.rem(me + count - step, count)).wait()
        return carry

    lax.fori_loop(1, count, give, 0)
    for copy in copies:
        copy.start()
    all_sums[me] = sum_ref[...]
    lax.fori_loop(1, count, take, 0)
    total = lax.fori_loop(
        0, count, lambda source, held: held + all_sums[source], jnp.zeros((8, LANES), jnp.float32)
    )
    virial = total[0:3]
    kinetic = total[3:6]
    energy = total[3:4] + total[4:5] + total[5:6]
    volume = box_ref[0] * box_ref[1] * box_ref[2]
    ratio = 2.0 * energy / (3.0 * particles * thermal_scale_unit)
    rate_ref[3:4] = extended_ref[0] + reservoir_inertia_mass * (ratio - 1.0)
    change = barostat_gain * (kinetic - virial - pressure_target * volume / 2.0) / (energy / 3.0)
    for c in range(3):
        rate_ref[c : c + 1] = extended_ref[1 + c] + change[c : c + 1]
    for copy in copies:
        copy.wait()


def returned(box_lengths, extended_variables, near, far, sums, count, particles):
    vmem = pl.BlockSpec(memory_space=pltpu.VMEM)
    smem = pl.BlockSpec(memory_space=pltpu.SMEM)
    return pl.pallas_call(
        functools.partial(return_kernel, count=count, particles=particles),
        name="return_kernel",
        out_shape=(
            jax.ShapeDtypeStruct(near.shape, near.dtype),
            jax.ShapeDtypeStruct(far.shape, far.dtype),
            jax.ShapeDtypeStruct((4, LANES), jnp.float32),
        ),
        in_specs=[smem] * 2 + [vmem] * 3,
        out_specs=(vmem,) * 3,
        scratch_shapes=[
            pltpu.VMEM((count, 8, LANES), jnp.float32),
            pltpu.SemaphoreType.DMA((2,)),
            pltpu.SemaphoreType.DMA((2,)),
            pltpu.SemaphoreType.DMA((count,)),
            pltpu.SemaphoreType.DMA((count,)),
        ],
        compiler_params=pltpu.CompilerParams(collective_id=1, has_side_effects=True),
    )(box_lengths, extended_variables, near, far, sums)


def on_device(
    positions,
    velocities,
    atom_params,
    pair_list,
    pair_count,
    exclusion,
    halo_far,
    box_lengths,
    extended_variables,
):
    atoms_here = positions.shape[1]
    clusters = atoms_here // 8
    far_clusters = halo_far.shape[0]
    slots = 2 * clusters + far_clusters
    axis_count = lax.axis_size("gx")
    packed, chosen = pack(positions, atom_params, halo_far)
    near_rows, beyond, picked = forward(packed, chosen, axis_count)
    lift = (lax.axis_index("gx") - (axis_count - 2)).astype(jnp.int32)[None]
    own, near, far, sums = pair_forces(
        (pair_count, box_lengths, lift),
        (packed, near_rows, beyond, picked, velocities, atom_params),
        pair_list, exclusion, clusters, slots,
    )
    near_back, far_back, rates = returned(
        box_lengths, extended_variables, near, far, sums, axis_count, atoms_here * axis_count
    )
    forces, new_velocities, new_positions, new_coupling = finished(
        own, near_back, far_back, rates, positions, velocities, atom_params
    )
    return (forces, new_velocities, new_positions, new_coupling.reshape(4))


def solution(mesh):
    return jax.shard_map(
        on_device,
        mesh=mesh,
        in_specs=(
            P(None, ("rep", "gx")),
            P(None, ("rep", "gx")),
            P(None, ("rep", "gx")),
            P(None, ("rep", "gx")),
            P(("rep", "gx")),
            P(None, ("rep", "gx")),
            P(("rep", "gx")),
            P("rep"),
            P("rep"),
        ),
        out_specs=(
            P(None, ("rep", "gx")),
            P(None, ("rep", "gx")),
            P(None, ("rep", "gx")),
            P("rep"),
        ),
        check_vma=False,
    )
```
